128 devices in a mesh: row: 16 (over y, z), col: 8 (over x, core).
Axes of the slice: x: 4, y: 4, z: 4, core: 2. Of those that a mesh axis runs over, the one named last changes fastest.
Arguments:
- front: bfloat16 [2, 32768, 6144], P(None, 'row', 'col'), may hold values from -6 to 6
- child_tiles: bfloat16 [16384, 2, 128, 128], P(('row', 'col')), may hold values from -6 to 6
- tile_owner: int32 [16384, 1], P(('row', 'col')), may hold values from 0 to 127; in each aligned block of 128 rows (0 to 127, 128 to 255, ...) at most 2 rows name the same one
- tile_spot: int32 [16384], P(('row', 'col')), may hold values from 0 to 95
- tile_count: int32 [128], P(('row', 'col')), may hold values from 96 to 128, as said below
- panel: bfloat16 [2, 32768, 512], P(None, 'row'), may hold values from -0.0234375 to 0.0234375
Outputs:
- assembled: bfloat16 [2, 32768, 6144], P(None, 'row', 'col')
- sample: float32 [2, 512, 6144], P(None, 'row', 'col')
The draws below stay inside these ranges and needn't reach their ends.
Inputs may be any that keep to these rules, and one draw needn't show every extreme that they name: `tile_owner`: among the 128 tiles of one device, at most 2 name the same owner. `tile_count`: some device holds 128 live tiles.
All inputs are finite; a program needn't handle non-finite values.
Results may differ from the reference program's by a relative error of at most 0.0042.
Values may be sent and summed in bfloat16 or wider, within the bound.
No kernel may reach another device: no remote copies, remote signals or barrier semaphores. Data moves between devices by JAX's collectives and lax.ppermute only.
A program may use at most 256 MiB of HBM per device.

```python
import math
import jax
import jax.numpy as jnp
import numpy as np
from jax import lax

TILE = 128
BR_DEV = 16
BC_DEV = 6
P_SIZE = 512
TILES_DEV = 128
NDEV = 128
CAP = 2
ROWS = 32768
COLS = 6144
N_COL = 8


def draw_tile_count(key, part):
    lowest = TILES_DEV - TILES_DEV // 4
    counts = jax.random.randint(jax.random.fold_in(key, 11), (NDEV,), lowest, TILES_DEV + 1, dtype=jnp.int32)
    fullest = jax.random.randint(jax.random.fold_in(key, 12), (), 0, NDEV, dtype=jnp.int32)
    return counts.at[fullest].set(TILES_DEV)


def set_ends(drawn, stream_key, smallest, top_value):
    longest = drawn.shape.index(max(drawn.shape))
    spots = []
    for shift in (0, 1):
        where = [jax.random.randint(jax.random.fold_in(stream_key, axis), (), 0, length) for axis, length in enumerate(drawn.shape)]
        where[longest] = (where[longest] + shift) % drawn.shape[longest]
        spots.append(tuple(where))
    return drawn.at[spots[0]].set(smallest).at[spots[1]].set(top_value)


def level_of(stream_key, shape, pieces, smallest, high):
    def one(dim, shards_of):
        draws = jax.random.uniform(jax.random.fold_in(jax.random.fold_in(stream_key, 6), dim), (shards_of,), jnp.float32, smallest / len(pieces), high / len(pieces))
        return jnp.repeat(jnp.exp(draws), shape[dim] // shards_of).reshape((-1,) + (1,) * (len(shape) - dim - 1))

    loudness = one(*pieces[0])
    for cut in pieces[1:]:
        loudness = loudness * one(*cut)
    return loudness


def routed_block(rng, own, number, rows, amount, top, reach, lean):
    order = jax.random.permutation(rng, amount)
    crowded, ordinary = load_shares(amount, rows * top, reach, lean, True), load_shares(amount, rows * top, reach, lean, False)
    places = jnp.arange(amount)

    def named(tallies, offset_by):
        used = int((tallies > 0).sum())
        fixed = max(1, used // 4)
        moved = fixed + (places - fixed + offset_by * (used - fixed)) % max(1, amount - fixed)
        return jnp.zeros((amount,), jnp.int32).at[order[jnp.where(places < fixed, places, moved)]].set(jnp.asarray(tallies, jnp.int32))

    tallies = jnp.where(number % 4 == 0, named(crowded, number // 4), named(ordinary, number - number // 4 - 1))
    mixed = jax.random.permutation(jax.random.fold_in(own, 3), amount)
    donor, sink = mixed[0:amount // 2 * 2:2], mixed[1:amount // 2 * 2:2]
    slack = jnp.minimum(tallies[donor] - 1, reach - tallies[sink]) // 2
    slack = jnp.where((donor == order[0]) | (sink == order[0]) | (tallies[sink] == 0), 0, jnp.maximum(slack, 0))
    moved = jax.random.randint(jax.random.fold_in(own, 4), (amount // 2,), 0, 1 << 20) % (slack + 1)
    tallies = tallies.at[donor].add(-moved).at[sink].add(moved)
    items = jnp.searchsorted(jnp.cumsum(tallies), jnp.arange(rows * top), side="right").astype(jnp.int32)
    grid = items.reshape(top, rows).T
    grid = grid[jax.random.permutation(jax.random.fold_in(own, 1), rows)]
    offset_by = jax.random.randint(jax.random.fold_in(own, 2), (rows, 1), 0, top)
    return jnp.take_along_axis(grid, (jnp.arange(top)[None, :] + offset_by) % top, axis=1)


def load_shares(count, total, reach, slope, full):
    weights = [(1 << 20) // math.isqrt(grade ** slope) + 1 for grade in range(1, count + 1)]
    largest = reach if full else min(reach, max(-(-total // count), total * weights[0] // sum(weights)))
    least = 1 if total - largest >= count - 1 else 0
    given, rest = [largest] + [least] * (count - 1), total - largest - least * (count - 1)
    while rest > 0:
        free = [i for i in range(1, count) if given[i] < largest] or [i for i in range(1, count) if given[i] < reach]
        whole, budget = sum([weights[i] for i in free]), rest
        for i in free:
            addition = min(reach - given[i], max(1, budget * weights[i] // whole), rest)
            given[i] = given[i] + addition
            rest = rest - addition
    return np.array(given)


def centred(key, shape, deviation, reach, cuts=(), kind=jnp.bfloat16):
    loudness = level_of(key, shape, cuts, -0.22, 0.18) if cuts else 1.0
    entries = jax.random.normal(key, shape, jnp.float32) * deviation * loudness
    return jnp.minimum(jnp.maximum(entries, -reach), reach).astype(kind)


def setup_inputs(seed: int = 0) -> dict:
    seeds = jax.random.split(jax.random.key(seed), 7)
    front = centred(seeds[0], (2, ROWS, COLS), 1.0, 6.0, ((1, 16), (2, 8)))
    child_tiles = centred(seeds[1], (NDEV * TILES_DEV, 2, TILE, TILE), 1.0, 6.0, ((0, 128),))
    tile_owner_keys = jax.random.split(jax.random.fold_in(seeds[2], 1), (NDEV * TILES_DEV) // TILES_DEV)
    tile_owner_turns = jax.random.permutation(jax.random.fold_in(seeds[2], 3), (NDEV * TILES_DEV) // TILES_DEV)
    tile_owner = jax.vmap(lambda own, number: routed_block(jax.random.fold_in(seeds[2], 2), own, number, TILES_DEV, NDEV, 1, CAP, 2))(tile_owner_keys, tile_owner_turns).reshape((NDEV * TILES_DEV, 1))
    tile_spot = set_ends(jax.random.randint(seeds[3], (NDEV * TILES_DEV,), 0, BR_DEV * BC_DEV), jax.random.fold_in(seeds[3], 1), 0, (BR_DEV * BC_DEV) - 1).astype(jnp.int32)
    tile_count = draw_tile_count(jax.random.fold_in(seeds[6], 71), 0)
    panel = centred(seeds[5], (2, ROWS, P_SIZE), (2 * ROWS) ** -0.5, 0.0234375, ((1, 16),))
    return {"front": front, "child_tiles": child_tiles, "tile_owner": tile_owner, "tile_spot": tile_spot, "tile_count": tile_count, "panel": panel}


def reference(front, child_tiles, tile_owner, tile_spot, tile_count, panel):
    total = child_tiles.shape[0]
    index = jnp.arange(total, dtype=jnp.int32)
    device = index // TILES_DEV
    live = (index % TILES_DEV) < tile_count[device]
    owner = tile_owner[:, 0]
    block_rows = ROWS // TILE
    block_cols = COLS // TILE
    target_row = (owner // N_COL) * BR_DEV + tile_spot // BC_DEV
    target_col = (owner % N_COL) * BC_DEV + tile_spot % BC_DEV
    target_row = jnp.where(live, target_row, block_rows).astype(jnp.int32)
    accum = front.astype(jnp.float32).reshape(2, block_rows, TILE, block_cols, TILE)
    tiles = child_tiles.reshape(NDEV, TILES_DEV, 2, TILE, TILE)
    rows_each = target_row.reshape(NDEV, TILES_DEV)
    cols_each = target_col.reshape(NDEV, TILES_DEV).astype(jnp.int32)

    def add_device(carry, item):
        piece, rows_here, cols_here = item
        carry = carry.at[:, rows_here, :, cols_here, :].add(piece.astype(jnp.float32), mode="drop")
        return carry, None

    accum, unused = lax.scan(add_device, accum, (tiles, rows_each, cols_each))
    assembled = accum.reshape(2, ROWS, COLS).astype(jnp.bfloat16)
    panel_re, panel_im = panel[0], panel[1]
    front_re, front_im = assembled[0], assembled[1]
    real_part = jnp.dot(panel_re.T, front_re, preferred_element_type=jnp.float32) + jnp.dot(panel_im.T, front_im, preferred_element_type=jnp.float32)
    imag_part = jnp.dot(panel_re.T, front_im, preferred_element_type=jnp.float32) - jnp.dot(panel_im.T, front_re, preferred_element_type=jnp.float32)
    return assembled, jnp.stack([real_part, imag_part])
```

```python
import functools

import jax
import jax.numpy as jnp
from jax import lax
from jax.experimental import pallas as pl
from jax.experimental.pallas import tpu as pltpu
from jax.sharding import PartitionSpec as P

BOTH = ("row", "col")
VMEM_LIMIT = 60 * 1024 * 1024


def pack(n_dev, chunk, owner, spot, count, tiles, out, meta, source, held, sem_in, sem_out, seen, sem_late):
    n_tiles = tiles.shape[0]

    def clear(d, carry):
        seen[d] = 0
        for k in range(2):
            meta[k * n_dev + d] = -1
            source[k * n_dev + d] = 0
        return carry

    lax.fori_loop(0, n_dev, clear, 0, unroll=8)

    def route(j, carry):
        to = owner[j]
        rank = seen[to]
        seen[to] = rank + 1
        meta[rank * n_dev + to] = spot[j]
        source[rank * n_dev + to] = j
        return carry

    lax.fori_loop(0, jnp.minimum(count[0], n_tiles), route, 0)

    chunks = n_dev // chunk

    def fetch(c, carry):
        def one(u, carry):
            d = c * chunk + u
            pltpu.make_async_copy(tiles.at[source[d]], held.at[d], sem_in.at[c]).start()
            return carry

        return lax.fori_loop(0, chunk, one, carry, unroll=4)

    lax.fori_loop(0, chunks, fetch, 0)

    def forward(c):
        part = pl.ds(c * chunk, chunk)
        return pltpu.make_async_copy(held.at[part], out.at[part, 0], sem_out.at[c])

    def drain(c, carry):
        part = pl.ds(c * chunk, chunk)
        pltpu.make_async_copy(tiles.at[pl.ds(0, chunk)], held.at[part], sem_in.at[c]).wait()
        forward(c).start()
        return carry

    def each(step):
        def one(d, carry):
            @pl.when(meta[n_dev + d] >= 0)
            def _():
                step(d)

            return carry

        lax.fori_loop(0, n_dev, one, 0, unroll=4)

    def fetch_late(d):
        return pltpu.make_async_copy(tiles.at[source[n_dev + d]], held.at[n_dev + d], sem_late.at[0, d])

    def forward_late(d):
        return pltpu.make_async_copy(held.at[n_dev + d], out.at[d, 1], sem_late.at[1, d])

    def pass_on(d):
        fetch_late(d).wait()
        forward_late(d).start()

    each(lambda d: fetch_late(d).start())
    lax.fori_loop(0, chunks, drain, 0)
    each(pass_on)

    def finish(c, carry):
        forward(c).wait()
        return carry

    lax.fori_loop(0, chunks, finish, 0)
    each(lambda d: forward_late(d).wait())


def extend_add(cols_blocks, ahead, order, starts, spots, front, tiles, assembled, held, block, sem):
    step = pl.program_id(0)
    steps = pl.num_programs(0)

    def fetch(p):
        return pltpu.make_async_copy(tiles.at[order[p]], held.at[p], sem.at[p])

    def begin(p, carry):
        fetch(p).start()
        return carry

    @pl.when(step == 0)
    def _():
        lax.fori_loop(0, starts[ahead], begin, 0)

    @pl.when(step + ahead < steps)
    def _():
        lax.fori_loop(starts[step + ahead], starts[step + ahead + 1], begin, 0)

    block[...] = front[...].astype(jnp.float32)

    def add(p, carry):
        fetch(p).wait()
        spot = spots[order[p]]
        column = pl.multiple_of((spot - step * cols_blocks) * 128, 128)
        for part in range(2):
            here = (part, slice(None), pl.ds(column, 128))
            block[here] += held[p, pl.ds(part * 128, 128), :].astype(jnp.float32)
        return carry

    lax.fori_loop(starts[step], starts[step + 1], add, 0)
    assembled[...] = block[...].astype(jnp.bfloat16)


def body(front, child_tiles, tile_owner, tile_spot, tile_count, panel):
    n_row = lax.axis_size("row")
    n_col = lax.axis_size("col")
    n_dev = n_row * n_col
    n_tiles = child_tiles.shape[0]
    tile = child_tiles.shape[2]
    height, width = front.shape[1:]
    rows_blocks, cols_blocks = height // tile, width // tile
    samples = panel.shape[2]
    f32, bf16, i32 = jnp.float32, jnp.bfloat16, jnp.int32
    smem = pl.BlockSpec(memory_space=pltpu.SMEM)
    hbm = pl.BlockSpec(memory_space=pl.ANY)
    params = functools.partial(pltpu.CompilerParams, vmem_limit_bytes=VMEM_LIMIT)
    tiles = child_tiles.reshape(n_tiles, 2 * tile, tile)
    chunk = 16
    n_slots = 2 * n_dev

    packed, meta, _ = pl.pallas_call(
        functools.partial(pack, n_dev, chunk),
        out_shape=(
            jax.ShapeDtypeStruct((n_dev, 2, 2 * tile, tile), bf16),
            jax.ShapeDtypeStruct((n_slots,), i32),
            jax.ShapeDtypeStruct((n_slots,), i32),
        ),
        in_specs=[smem, smem, smem, hbm],
        out_specs=(hbm, smem, smem),
        scratch_shapes=[
            pltpu.VMEM((n_slots, 2 * tile, tile), bf16),
            pltpu.SemaphoreType.DMA((n_dev // chunk,)),
            pltpu.SemaphoreType.DMA((n_dev // chunk,)),
            pltpu.SMEM((n_dev,), i32),
            pltpu.SemaphoreType.DMA((2, n_dev)),
        ],
        compiler_params=params(),
        cost_estimate=pl.CostEstimate(flops=1 << 20, bytes_accessed=2 * n_dev * 65536, transcendentals=0),
        name="pack",
    )(tile_owner[:, 0], tile_spot, tile_count, tiles)
    got = lax.all_to_all(packed, BOTH, split_axis=0, concat_axis=0, tiled=True)
    all_meta = lax.all_gather(meta.reshape(2, n_dev), BOTH, axis=0, tiled=False)
    me = lax.axis_index("row") * n_col + lax.axis_index("col")
    spots = lax.dynamic_index_in_dim(all_meta, me, axis=2, keepdims=False).reshape(n_slots)

    slot = jnp.arange(n_slots, dtype=i32)
    block_of = jnp.where(spots >= 0, spots // cols_blocks, rows_blocks)
    key = block_of * n_slots + slot
    place = jnp.sum((key[None, :] < key[:, None]).astype(i32), axis=1)
    order = jnp.sum(jnp.where(place[None, :] == slot[:, None], slot[None, :], 0), axis=1)
    starts = jnp.sum((block_of[None, :] < jnp.arange(rows_blocks + 1)[:, None]).astype(i32), axis=1)

    side = 4
    row = lax.axis_index("row")
    hop = jnp.arange(n_row, dtype=i32)
    target = (row // side + hop // side) % (n_row // side) * side + (row % side + hop % side) % side
    turned = panel.transpose(2, 0, 1)
    crossed = jnp.stack([-turned[:, 1], turned[:, 0]], axis=1)
    weights = jnp.stack([turned.reshape(n_row, -1, 2 * height), crossed.reshape(n_row, -1, 2 * height)], axis=1)
    weights = weights.reshape(n_row, 2 * samples // n_row, 2 * height)[target]

    ahead = 2
    assembled = pl.pallas_call(
        functools.partial(extend_add, cols_blocks, ahead),
        grid=(rows_blocks,),
        out_shape=jax.ShapeDtypeStruct((2, height, width), bf16),
        in_specs=[
            smem,
            smem,
            smem,
            pl.BlockSpec((2, tile, width), lambda i: (0, i, 0)),
            hbm,
        ],
        out_specs=pl.BlockSpec((2, tile, width), lambda i: (0, i, 0)),
        scratch_shapes=[
            pltpu.VMEM((n_slots, 2 * tile, tile), bf16),
            pltpu.VMEM((2, tile, width), f32),
            pltpu.SemaphoreType.DMA((n_slots,)),
        ],
        compiler_params=params(),
        cost_estimate=pl.CostEstimate(flops=8 << 30, bytes_accessed=28 << 20, transcendentals=0),
        name="extend_add",
    )(order, starts, spots, front, got.reshape(n_slots, 2 * tile, tile))

    stacked = assembled.reshape(2 * height, width)
    groups = 4
    each = n_row // groups
    received = []
    for g in range(groups):
        part = weights[g * each : (g + 1) * each].reshape(-1, 2 * height)
        part = jnp.dot(part, stacked, preferred_element_type=f32).astype(bf16)
        part = part.reshape(each, -1, width)
        for k in range(each):
            h = g * each + k
            if h == 0:
                received.append(part[k])
                continue
            pairs = []
            for r in range(n_row):
                to = (r // side + h // side) % (n_row // side) * side + (r % side + h % side) % side
                pairs.append((r, to))
            received.append(lax.ppermute(part[k], "row", pairs))
    sample = sum(x.astype(f32) for x in received)
    return assembled, sample.reshape(2, samples // n_row, width)


def solution(mesh):
    placed = (
        P(None, "row", "col"),
        P(BOTH, None, None, None),
        P(BOTH, None),
        P(BOTH),
        P(BOTH),
        P(None, "row", None),
    )
    return jax.shard_map(
        body,
        mesh=mesh,
        in_specs=placed,
        out_specs=(P(None, "row", "col"), P(None, "row", "col")),
        check_vma=False,
    )
```

```python
import functools

import jax
import jax.numpy as jnp
from jax import lax
from jax.experimental import pallas as pl
from jax.experimental.pallas import tpu as pltpu
from jax.sharding import PartitionSpec as P

BOTH = ("row", "col")
VMEM_LIMIT = 60 * 1024 * 1024


def pack(n_dev, owner, spot, count, tiles, out, held, labels, sem_in, sem_out, sem_labels, seen, slot_of, spots):
    live = jnp.minimum(count[0], tiles.shape[0])

    def clear(d, carry):
        seen[d] = 0
        for k in range(2):
            spots[d * 2 + k] = -1
        return carry

    lax.fori_loop(0, n_dev, clear, 0, unroll=8)

    def fetch(j):
        return pltpu.make_async_copy(tiles.at[j], held.at[j], sem_in.at[j])

    def forward(j):
        slot = slot_of[j]
        to = slot // 2
        here = out.at[to, pl.ds(pl.multiple_of((slot - to * 2) * 256, 256), 256)]
        return pltpu.make_async_copy(held.at[j], here, sem_out.at[j])

    def route(j, carry):
        fetch(j).start()
        to = owner[j]
        rank = seen[to]
        seen[to] = rank + 1
        slot_of[j] = to * 2 + rank
        spots[to * 2 + rank] = spot[j]
        return carry

    lax.fori_loop(0, live, route, 0)

    def pass_on(j, carry):
        fetch(j).wait()
        forward(j).start()
        return carry

    lax.fori_loop(0, live, pass_on, 0)
    lane = lax.broadcasted_iota(jnp.int32, (8, 128), 1)

    def label(d, carry):
        row = jnp.where(lane == 0, spots[d * 2], jnp.where(lane == 1, spots[d * 2 + 1], 0))
        labels[d] = row.astype(jnp.float32).astype(jnp.bfloat16)
        return carry

    lax.fori_loop(0, n_dev, label, 0, unroll=4)
    send_labels = pltpu.make_async_copy(labels, out.at[:, pl.ds(512, 8)], sem_labels)
    send_labels.start()

    def finish(j, carry):
        forward(j).wait()
        return carry

    lax.fori_loop(0, live, finish, 0)
    send_labels.wait()


def extend_add(cols_blocks, ahead, order, starts, front, tiles, assembled, held, sem):
    step = pl.program_id(0)
    steps = pl.num_programs(0)

    def fetch(p):
        slot = order[p]
        source = slot // 2
        here = tiles.at[source, pl.ds(pl.multiple_of((slot - source * 2) * 256, 256), 256)]
        return pltpu.make_async_copy(here, held.at[p], sem.at[p])

    def begin(p, carry):
        fetch(p).start()
        return carry

    def arrive(p, carry):
        fetch(p).wait()
        return carry

    def fence(s):
        return starts[s * cols_blocks]

    @pl.when(step == 0)
    def _():
        lax.fori_loop(0, fence(ahead), begin, 0)

    @pl.when(step + ahead < steps)
    def _():
        lax.fori_loop(fence(step + ahead), fence(step + ahead + 1), begin, 0)

    lax.fori_loop(fence(step), fence(step + 1), arrive, 0)
    for c in range(cols_blocks):
        first, last = starts[step * cols_blocks + c], starts[step * cols_blocks + c + 1]
        for part in range(2):

            def add(p, value):
                return value + held[p, part * 128 : (part + 1) * 128, :].astype(jnp.float32)

            here = (part, slice(None), slice(c * 128, (c + 1) * 128))
            value = lax.fori_loop(first, last, add, front[here].astype(jnp.float32))
            assembled[here] = value.astype(jnp.bfloat16)


def body(front, child_tiles, tile_owner, tile_spot, tile_count, panel):
    n_row = lax.axis_size("row")
    n_dev = n_row * lax.axis_size("col")
    n_tiles = child_tiles.shape[0]
    tile = child_tiles.shape[2]
    height, width = front.shape[1:]
    rows_blocks, cols_blocks = height // tile, width // tile
    n_spots = rows_blocks * cols_blocks
    samples = panel.shape[2]
    f32, bf16, i32 = jnp.float32, jnp.bfloat16, jnp.int32
    smem = pl.BlockSpec(memory_space=pltpu.SMEM)
    hbm = pl.BlockSpec(memory_space=pl.ANY)
    params = functools.partial(pltpu.CompilerParams, vmem_limit_bytes=VMEM_LIMIT)
    n_slots = 2 * n_dev
    message = 4 * tile + 8

    packed = pl.pallas_call(
        functools.partial(pack, n_dev),
        out_shape=jax.ShapeDtypeStruct((n_dev, message, tile), bf16),
        in_specs=[smem, smem, smem, hbm],
        out_specs=hbm,
        scratch_shapes=[
            pltpu.VMEM((n_tiles, 2 * tile, tile), bf16),
            pltpu.VMEM((n_dev, 8, tile), bf16),
            pltpu.SemaphoreType.DMA((n_tiles,)),
            pltpu.SemaphoreType.DMA((n_tiles,)),
            pltpu.SemaphoreType.DMA,
            pltpu.SMEM((n_dev,), i32),
            pltpu.SMEM((n_tiles,), i32),
            pltpu.SMEM((n_slots,), i32),
        ],
        compiler_params=params(),
        cost_estimate=pl.CostEstimate(flops=1 << 20, bytes_accessed=2 * n_dev * 65536, transcendentals=0),
        name="pack",
    )(tile_owner[:, 0], tile_spot, tile_count, child_tiles.reshape(n_tiles, 2 * tile, tile))
    got = lax.all_to_all(packed, BOTH, split_axis=0, concat_axis=0, tiled=True)

    spots = got[:, 4 * tile, :2].astype(i32).reshape(n_slots)
    slot = jnp.arange(n_slots, dtype=i32)
    key = jnp.where(spots >= 0, spots, n_spots) * n_slots + slot
    place = jnp.sum((key[None, :] < key[:, None]).astype(i32), axis=1)
    order = jnp.sum(jnp.where(place[None, :] == slot[:, None], slot[None, :], 0), axis=1)
    starts = jnp.sum((key[None, :] < (jnp.arange(n_spots + 1) * n_slots)[:, None]).astype(i32), axis=1)

    turned = panel.transpose(2, 0, 1)
    crossed = jnp.stack([-turned[:, 1], turned[:, 0]], axis=1)
    weights = jnp.stack([turned.reshape(n_row, -1, 2 * height), crossed.reshape(n_row, -1, 2 * height)], axis=1)
    weights = weights.reshape(2 * samples, 2 * height)

    ahead = 2
    assembled = pl.pallas_call(
        functools.partial(extend_add, cols_blocks, ahead),
        grid=(rows_blocks,),
        out_shape=jax.ShapeDtypeStruct((2, height, width), bf16),
        in_specs=[
            smem,
            smem,
            pl.BlockSpec((2, tile, width), lambda i: (0, i, 0)),
            hbm,
        ],
        out_specs=pl.BlockSpec((2, tile, width), lambda i: (0, i, 0)),
        scratch_shapes=[
            pltpu.VMEM((n_slots, 2 * tile, tile), bf16),
            pltpu.SemaphoreType.DMA((n_slots,)),
        ],
        compiler_params=params(),
        cost_estimate=pl.CostEstimate(flops=8 << 30, bytes_accessed=28 << 20, transcendentals=0),
        name="extend_add",
    )(order, starts, front, got)

    partial = jnp.dot(weights, assembled.reshape(2 * height, width), preferred_element_type=f32).astype(bf16)
    arrived = lax.all_to_all(
        partial.reshape(n_row, 2 * samples // n_row, width), "row", split_axis=0, concat_axis=0, tiled=True
    )
    sample = arrived.astype(f32).sum(axis=0).reshape(2, samples // n_row, width)
    return assembled, sample


def solution(mesh):
    placed = (
        P(None, "row", "col"),
        P(BOTH, None, None, None),
        P(BOTH, None),
        P(BOTH),
        P(BOTH),
        P(None, "row", None),
    )
    return jax.shard_map(
        body,
        mesh=mesh,
        in_specs=placed,
        out_specs=(P(None, "row", "col"), P(None, "row", "col")),
        check_vma=False,
    )
```

```python
import functools

import jax
import jax.numpy as jnp
from jax import lax
from jax.experimental import pallas as pl
from jax.experimental.pallas import tpu as pltpu
from jax.sharding import PartitionSpec as P

BOTH = ("row", "col")
VMEM_LIMIT = 4 * 1024 * 1024


def pack(n_dev, owner, spot, count, tiles, out, sem, seen, slot_of, spots):
    live = jnp.minimum(count[0], tiles.shape[0])

    def clear(d, carry):
        seen[d] = 0
        for k in range(2):
            spots[d * 2 + k] = -1
        return carry

    lax.fori_loop(0, n_dev, clear, 0, unroll=8)

    def fetch(j, to, rank):
        here = out.at[to, pl.ds(pl.multiple_of(rank * 256, 256), 256)]
        return pltpu.make_async_copy(tiles.at[j], here, sem.at[j])

    def route(j, carry):
        to = owner[j]
        rank = seen[to]
        fetch(j, to, rank).start()
        seen[to] = rank + 1
        slot_of[j] = to * 2 + rank
        spots[to * 2 + rank] = spot[j]
        return carry

    lax.fori_loop(0, live, route, 0)
    lane = lax.broadcasted_iota(jnp.int32, (8, 128), 1)

    def label(d, carry):
        row = jnp.where(lane == 0, spots[d * 2], jnp.where(lane == 1, spots[d * 2 + 1], 0))
        out[d, 512:520, :] = row.astype(jnp.float32).astype(jnp.bfloat16)
        return carry

    lax.fori_loop(0, n_dev, label, 0, unroll=4)

    def finish(j, carry):
        slot = slot_of[j]
        to = slot // 2
        fetch(j, to, slot - to * 2).wait()
        return carry

    lax.fori_loop(0, live, finish, 0)


def extend_add(n_dev, rows_blocks, cols_blocks, order, starts, tiles, front, assembled, rounded, sem):
    def rows(step):
        return pl.ds(pl.multiple_of(step * 128, 128), 128)

    def put(step):
        turn = step % 2
        return pltpu.make_async_copy(rounded.at[turn], assembled.at[:, rows(step)], sem.at[turn])

    def one(step, carry):
        turn = step % 2

        @pl.when(step >= 2)
        def _():
            put(step - 2).wait()

        for c in range(cols_blocks):
            first, last = starts[step * cols_blocks + c], starts[step * cols_blocks + c + 1]
            columns = slice(c * 128, (c + 1) * 128)
            for part in range(2):

                def add(p, value):
                    slot = order[p]
                    rank = slot // n_dev
                    here = pl.ds(pl.multiple_of(rank * 256 + part * 128, 128), 128)
                    return value + tiles[slot - rank * n_dev, here, :].astype(jnp.float32)

                value = lax.fori_loop(first, last, add, front[part, rows(step), columns].astype(jnp.float32))
                rounded[turn, part, :, columns] = value.astype(jnp.bfloat16)
        put(step).start()
        return carry

    lax.fori_loop(0, rows_blocks, one, 0)
    for step in (rows_blocks - 2, rows_blocks - 1):
        put(step).wait()


def body(front, child_tiles, tile_owner, tile_spot, tile_count, panel):
    n_row = lax.axis_size("row")
    n_dev = n_row * lax.axis_size("col")
    n_tiles = child_tiles.shape[0]
    tile = child_tiles.shape[2]
    height, width = front.shape[1:]
    rows_blocks, cols_blocks = height // tile, width // tile
    n_spots = rows_blocks * cols_blocks
    samples = panel.shape[2]
    f32, bf16, i32 = jnp.float32, jnp.bfloat16, jnp.int32
    smem = pl.BlockSpec(memory_space=pltpu.SMEM)
    hbm = pl.BlockSpec(memory_space=pltpu.HBM)
    vmem = pl.BlockSpec(memory_space=pltpu.VMEM)
    params = functools.partial(pltpu.CompilerParams, vmem_limit_bytes=VMEM_LIMIT)
    n_slots = 2 * n_dev
    message = 4 * tile + 8

    packed = pl.pallas_call(
        functools.partial(pack, n_dev),
        out_shape=jax.ShapeDtypeStruct((n_dev, message, tile), bf16),
        in_specs=[smem, smem, smem, hbm],
        out_specs=vmem,
        scratch_shapes=[
            pltpu.SemaphoreType.DMA((n_tiles,)),
            pltpu.SMEM((n_dev,), i32),
            pltpu.SMEM((n_tiles,), i32),
            pltpu.SMEM((n_slots,), i32),
        ],
        compiler_params=params(),
        cost_estimate=pl.CostEstimate(flops=1 << 20, bytes_accessed=2 * n_dev * 65536, transcendentals=0),
        name="pack",
    )(tile_owner[:, 0], tile_spot, tile_count, child_tiles.reshape(n_tiles, 2 * tile, tile))
    got = lax.all_to_all(packed, BOTH, split_axis=0, concat_axis=0, tiled=True)

    spots = jnp.concatenate([got[:, 4 * tile, 0], got[:, 4 * tile, 1]]).astype(i32)
    slot = jnp.arange(n_slots, dtype=i32)
    spots = jnp.where(spots >= 0, spots, n_spots)
    key = spots * n_slots + slot
    place = jnp.sum((key[None, :] < key[:, None]).astype(i32), axis=1)
    order = jnp.sum(jnp.where(place[None, :] == slot[:, None], slot[None, :], 0), axis=1)
    starts = jnp.sum((spots[None, :] < jnp.arange(n_spots + 1)[:, None]).astype(i32), axis=1)

    assembled = pl.pallas_call(
        functools.partial(extend_add, n_dev, rows_blocks, cols_blocks),
        out_shape=jax.ShapeDtypeStruct((2, height, width), bf16),
        in_specs=[smem, smem, vmem, vmem],
        out_specs=hbm,
        scratch_shapes=[
            pltpu.VMEM((2, 2, tile, width), bf16),
            pltpu.SemaphoreType.DMA((2,)),
        ],
        compiler_params=params(),
        cost_estimate=pl.CostEstimate(flops=8 << 30, bytes_accessed=28 << 20, transcendentals=0),
        name="extend_add",
    )(order, starts, got, front)

    def product(p, a):
        return lax.dot_general(p, a, (((0,), (0,)), ((), ())), preferred_element_type=f32)

    real = product(panel.reshape(2 * height, samples), assembled.reshape(2 * height, width))
    imag = product(panel[0], assembled[1]) - product(panel[1], assembled[0])
    partial = jnp.stack([real.astype(bf16).reshape(n_row, -1, width), imag.astype(bf16).reshape(n_row, -1, width)], axis=1)
    arrived = lax.all_to_all(
        partial.reshape(n_row, 2 * samples // n_row, width), "row", split_axis=0, concat_axis=0, tiled=True
    )
    sample = arrived.astype(f32).sum(axis=0).reshape(2, samples // n_row, width)
    return assembled, sample


def solution(mesh):
    placed = (
        P(None, "row", "col"),
        P(BOTH, None, None, None),
        P(BOTH, None),
        P(BOTH),
        P(BOTH),
        P(None, "row", None),
    )
    return jax.shard_map(
        body,
        mesh=mesh,
        in_specs=placed,
        out_specs=(P(None, "row", "col"), P(None, "row", "col")),
        check_vma=False,
    )
```

```python
import functools

import jax
import jax.numpy as jnp
from jax import lax
from jax.experimental import pallas as pl
from jax.experimental.pallas import tpu as pltpu
from jax.sharding import PartitionSpec as P

BOTH = ("row", "col")
VMEM_LIMIT = 4 * 1024 * 1024


def pack(n_dev, owner, spot, count, tiles, out, seen, spots):
    def clear(d, carry):
        seen[d] = 0
        for k in range(2):
            spots[d * 2 + k] = -1
        return carry

    lax.fori_loop(0, n_dev, clear, 0, unroll=8)

    def route(j, carry):
        to = owner[j]
        rank = seen[to]
        seen[to] = rank + 1
        spots[to * 2 + rank] = spot[j]
        out[to, pl.ds(pl.multiple_of(rank * 256, 256), 256), :] = tiles[j]
        return carry

    lax.fori_loop(0, jnp.minimum(count[0], tiles.shape[0]), route, 0)
    lane = lax.broadcasted_iota(jnp.int32, (8, 128), 1)

    def label(d, carry):
        row = jnp.where(lane == 0, spots[d * 2], jnp.where(lane == 1, spots[d * 2 + 1], 0))
        out[d, 512:520, :] = row.astype(jnp.float32).astype(jnp.bfloat16)
        return carry

    lax.fori_loop(0, n_dev, label, 0, unroll=4)


def extend_add(n_dev, rows_blocks, cols_blocks, order, starts, tiles, front, assembled, near, sem):
    def rows(step):
        return pl.ds(pl.multiple_of(step * 128, 128), 128)

    def put(step):
        return pltpu.make_async_copy(near.at[:, rows(step)], assembled.at[:, rows(step)], sem.at[step])

    def one(step, carry):
        for c in range(cols_blocks):
            first, last = starts[step * cols_blocks + c], starts[step * cols_blocks + c + 1]
            columns = slice(c * 128, (c + 1) * 128)

            def add(p, values):
                slot = order[p]
                rank = slot // n_dev
                source = slot - rank * n_dev
                return tuple(
                    value + tiles[source, pl.ds(pl.multiple_of(rank * 256 + part * 128, 128), 128), :].astype(jnp.float32)
                    for part, value in enumerate(values)
                )

            values = tuple(front[part, rows(step), columns].astype(jnp.float32) for part in range(2))
            for part, value in enumerate(lax.fori_loop(first, last, add, values)):
                near[part, rows(step), columns] = value.astype(jnp.bfloat16)
        put(step).start()
        return carry

    def finish(step, carry):
        put(step).wait()
        return carry

    lax.fori_loop(0, rows_blocks, one, 0)
    lax.fori_loop(0, rows_blocks, finish, 0)


def body(front, child_tiles, tile_owner, tile_spot, tile_count, panel):
    n_row = lax.axis_size("row")
    n_dev = n_row * lax.axis_size("col")
    n_tiles = child_tiles.shape[0]
    tile = child_tiles.shape[2]
    height, width = front.shape[1:]
    rows_blocks, cols_blocks = height // tile, width // tile
    n_spots = rows_blocks * cols_blocks
    samples = panel.shape[2]
    f32, bf16, i32 = jnp.float32, jnp.bfloat16, jnp.int32
    smem = pl.BlockSpec(memory_space=pltpu.SMEM)
    vmem = pl.BlockSpec(memory_space=pltpu.VMEM)
    params = functools.partial(pltpu.CompilerParams, vmem_limit_bytes=VMEM_LIMIT)
    n_slots = 2 * n_dev
    message = 4 * tile + 8

    packed = pl.pallas_call(
        functools.partial(pack, n_dev),
        out_shape=jax.ShapeDtypeStruct((n_dev, message, tile), bf16),
        in_specs=[smem, smem, smem, vmem],
        out_specs=vmem,
        scratch_shapes=[pltpu.SMEM((n_dev,), i32), pltpu.SMEM((n_slots,), i32)],
        compiler_params=params(),
        cost_estimate=pl.CostEstimate(flops=1 << 20, bytes_accessed=2 * n_dev * 65536, transcendentals=0),
        name="pack",
    )(tile_owner[:, 0], tile_spot, tile_count, child_tiles.reshape(n_tiles, 2 * tile, tile))
    got = lax.all_to_all(packed, BOTH, split_axis=0, concat_axis=0, tiled=True)

    spots = jnp.concatenate([got[:, 4 * tile, 0], got[:, 4 * tile, 1]]).astype(i32)
    slot = jnp.arange(n_slots, dtype=i32)
    spots = jnp.where(spots >= 0, spots, n_spots)
    key = spots * n_slots + slot
    place = jnp.sum((key[None, :] < key[:, None]).astype(i32), axis=1)
    order = jnp.sum(jnp.where(place[None, :] == slot[:, None], slot[None, :], 0), axis=1)
    starts = jnp.sum((spots[None, :] < jnp.arange(n_spots + 1)[:, None]).astype(i32), axis=1)

    result = jax.ShapeDtypeStruct((2, height, width), bf16)
    assembled, near = pl.pallas_call(
        functools.partial(extend_add, n_dev, rows_blocks, cols_blocks),
        out_shape=(result, result),
        in_specs=[smem, smem, vmem, vmem],
        out_specs=(pl.BlockSpec(memory_space=pl.ANY), vmem),
        scratch_shapes=[pltpu.SemaphoreType.DMA((rows_blocks,))],
        compiler_params=params(),
        cost_estimate=pl.CostEstimate(flops=8 << 30, bytes_accessed=28 << 20, transcendentals=0),
        name="extend_add",
    )(order, starts, got, front)

    def product(p, a):
        return lax.dot_general(p, a, (((0,), (0,)), ((), ())), preferred_element_type=f32)

    real = product(panel.reshape(2 * height, samples), near.reshape(2 * height, width))
    imag = product(panel[0], near[1]) - product(panel[1], near[0])
    partial = jnp.stack([real.astype(bf16).reshape(n_row, -1, width), imag.astype(bf16).reshape(n_row, -1, width)], axis=1)
    arrived = lax.all_to_all(
        partial.reshape(n_row, 2 * samples // n_row, width), "row", split_axis=0, concat_axis=0, tiled=True
    )
    sample = arrived.astype(f32).sum(axis=0).reshape(2, samples // n_row, width)
    return assembled, sample


def solution(mesh):
    placed = (
        P(None, "row", "col"),
        P(BOTH, None, None, None),
        P(BOTH, None),
        P(BOTH),
        P(BOTH),
        P(None, "row", None),
    )
    return jax.shard_map(
        body,
        mesh=mesh,
        in_specs=placed,
        out_specs=(P(None, "row", "col"), P(None, "row", "col")),
        check_vma=False,
    )
```

```python
import functools

import jax
import jax.numpy as jnp
from jax import lax
from jax.experimental import pallas as pl
from jax.experimental.pallas import tpu as pltpu
from jax.sharding import PartitionSpec as P

BOTH = ("row", "col")
VMEM_LIMIT = 4 * 1024 * 1024


def pack(n_dev, n_spots, target, count, tiles, out, seen, spots):
    def clear(d, carry):
        seen[d] = 0
        for k in range(2):
            spots[d * 2 + k] = -1
        return carry

    lax.fori_loop(0, n_dev, clear, 0, unroll=8)

    def route(j, carry):
        to = target[j] // n_spots
        rank = seen[to]
        seen[to] = rank + 1
        spots[to * 2 + rank] = target[j] - to * n_spots
        out[to, pl.ds(pl.multiple_of(rank * 256, 256), 256), :] = tiles[j]
        return carry

    lax.fori_loop(0, jnp.minimum(count[0], tiles.shape[0]), route, 0)
    lane = lax.broadcasted_iota(jnp.int32, (8, 128), 1)

    def label(d, carry):
        row = jnp.where(lane == 0, spots[d * 2], jnp.where(lane == 1, spots[d * 2 + 1], 0))
        out[d, 512:520, :] = row.astype(jnp.float32).astype(jnp.bfloat16)
        return carry

    lax.fori_loop(0, n_dev, label, 0, unroll=4)


def extend_add(n_dev, rows_blocks, cols_blocks, order, starts, tiles, front, assembled, near, sem):
    def rows(step):
        return pl.ds(pl.multiple_of(step * 128, 128), 128)

    def put(step):
        return pltpu.make_async_copy(near.at[:, rows(step)], assembled.at[:, rows(step)], sem.at[step])

    def one(step, carry):
        for c in range(cols_blocks):
            first, last = starts[step * cols_blocks + c], starts[step * cols_blocks + c + 1]
            columns = slice(c * 128, (c + 1) * 128)

            def add(p, carry):
                slot, values = carry
                rank = slot // n_dev
                source = slot - rank * n_dev
                return order[p + 1], tuple(
                    value + tiles[source, pl.ds(pl.multiple_of(rank * 256 + part * 128, 128), 128), :].astype(jnp.float32)
                    for part, value in enumerate(values)
                )

            values = tuple(front[part, rows(step), columns].astype(jnp.float32) for part in range(2))
            for part, value in enumerate(lax.fori_loop(first, last, add, (order[first], values))[1]):
                near[part, rows(step), columns] = value.astype(jnp.bfloat16)
        put(step).start()
        return carry

    def finish(step, carry):
        put(step).wait()
        return carry

    lax.fori_loop(0, rows_blocks, one, 0)
    lax.fori_loop(0, rows_blocks, finish, 0)


def body(front, child_tiles, tile_owner, tile_spot, tile_count, panel):
    n_row = lax.axis_size("row")
    n_dev = n_row * lax.axis_size("col")
    n_tiles = child_tiles.shape[0]
    tile = child_tiles.shape[2]
    height, width = front.shape[1:]
    rows_blocks, cols_blocks = height // tile, width // tile
    n_spots = rows_blocks * cols_blocks
    samples = panel.shape[2]
    f32, bf16, i32 = jnp.float32, jnp.bfloat16, jnp.int32
    smem = pl.BlockSpec(memory_space=pltpu.SMEM)
    vmem = pl.BlockSpec(memory_space=pltpu.VMEM)
    params = functools.partial(pltpu.CompilerParams, vmem_limit_bytes=VMEM_LIMIT)
    n_slots = 2 * n_dev
    message = 4 * tile + 8
    spot_range = pl.next_power_of_2(n_spots)

    packed = pl.pallas_call(
        functools.partial(pack, n_dev, spot_range),
        out_shape=jax.ShapeDtypeStruct((n_dev, message, tile), bf16),
        in_specs=[smem, smem, vmem],
        out_specs=vmem,
        scratch_shapes=[pltpu.SMEM((n_dev,), i32), pltpu.SMEM((n_slots,), i32)],
        compiler_params=params(),
        cost_estimate=pl.CostEstimate(flops=1 << 20, bytes_accessed=2 * n_dev * 65536, transcendentals=0),
        name="pack",
    )(tile_owner[:, 0] * spot_range + tile_spot, tile_count, child_tiles.reshape(n_tiles, 2 * tile, tile))
    got = lax.all_to_all(packed, BOTH, split_axis=0, concat_axis=0, tiled=True)

    spots = jnp.concatenate([got[:, 4 * tile, 0], got[:, 4 * tile, 1]]).astype(i32)
    slot = jnp.arange(n_slots, dtype=i32)
    spots = jnp.where(spots >= 0, spots, n_spots)
    key = spots * n_slots + slot
    place = jnp.sum((key[None, :] < key[:, None]).astype(i32), axis=1)
    order = jnp.sum(jnp.where(place[None, :] == jnp.arange(n_slots + 1)[:, None], slot[None, :], 0), axis=1)
    starts = jnp.sum((spots[None, :] < jnp.arange(n_spots + 1)[:, None]).astype(i32), axis=1)

    result = jax.ShapeDtypeStruct((2, height, width), bf16)
    assembled, near = pl.pallas_call(
        functools.partial(extend_add, n_dev, rows_blocks, cols_blocks),
        out_shape=(result, result),
        in_specs=[smem, smem, vmem, vmem],
        out_specs=(pl.BlockSpec(memory_space=pl.ANY), vmem),
        scratch_shapes=[pltpu.SemaphoreType.DMA((rows_blocks,))],
        compiler_params=params(),
        cost_estimate=pl.CostEstimate(flops=8 << 30, bytes_accessed=28 << 20, transcendentals=0),
        name="extend_add",
    )(order, starts, got, front)

    def product(p, a):
        return lax.dot_general(p, a, (((0,), (0,)), ((), ())), preferred_element_type=f32)

    real = product(panel[0], near[0]) + product(panel[1], near[1])
    imag = product(panel[0], near[1]) - product(panel[1], near[0])
    partial = jnp.stack([real.astype(bf16).reshape(n_row, -1, width), imag.astype(bf16).reshape(n_row, -1, width)], axis=1)
    arrived = lax.all_to_all(
        partial.reshape(n_row, 2 * samples // n_row, width), "row", split_axis=0, concat_axis=0, tiled=True
    )
    sample = arrived.astype(f32).sum(axis=0).reshape(2, samples // n_row, width)
    return assembled, sample


def solution(mesh):
    placed = (
        P(None, "row", "col"),
        P(BOTH, None, None, None),
        P(BOTH, None),
        P(BOTH),
        P(BOTH),
        P(None, "row", None),
    )
    return jax.shard_map(
        body,
        mesh=mesh,
        in_specs=placed,
        out_specs=(P(None, "row", "col"), P(None, "row", "col")),
        check_vma=False,
    )
```

```python
import functools

import jax
import jax.numpy as jnp
from jax import lax
from jax.experimental import pallas as pl
from jax.experimental.pallas import tpu as pltpu
from jax.sharding import PartitionSpec as P

BOTH = ("row", "col")
VMEM_LIMIT = 4 * 1024 * 1024


def pack(n_dev, n_spots, target, count, tiles, out, seen, spots):
    def clear(d, carry):
        seen[d] = 0
        for k in range(2):
            spots[d * 2 + k] = -1
        return carry

    lax.fori_loop(0, n_dev, clear, 0, unroll=8)

    def route(j, carry):
        to = target[j] // n_spots
        rank = seen[to]
        seen[to] = rank + 1
        spots[to * 2 + rank] = target[j] - to * n_spots
        out[to, pl.ds(pl.multiple_of(rank * 256, 256), 256), :] = tiles[j]
        return carry

    live = jnp.minimum(count[0], tiles.shape[0])
    lax.fori_loop(0, live // 4, lambda i, carry: functools.reduce(lambda c, u: route(i * 4 + u, c), range(4), carry), 0)
    lax.fori_loop(live // 4 * 4, live, route, 0)
    lane = lax.broadcasted_iota(jnp.int32, (8, 128), 1)

    def label(d, carry):
        row = jnp.where(lane == 0, spots[d * 2], jnp.where(lane == 1, spots[d * 2 + 1], 0))
        out[d, 512:520, :] = row.astype(jnp.float32).astype(jnp.bfloat16)
        return carry

    lax.fori_loop(0, n_dev, label, 0, unroll=4)


def extend_add(n_dev, rows_blocks, cols_blocks, order, starts, tiles, front, assembled, near, sem):
    def rows(step):
        return pl.ds(pl.multiple_of(step * 128, 128), 128)

    def put(step):
        return pltpu.make_async_copy(near.at[:, rows(step)], assembled.at[:, rows(step)], sem.at[step])

    def one(step, carry):
        for c in range(cols_blocks):
            first, last = starts[step * cols_blocks + c], starts[step * cols_blocks + c + 1]
            columns = slice(c * 128, (c + 1) * 128)

            def read(slot, part):
                rank = slot // n_dev
                here = pl.ds(pl.multiple_of(rank * 256 + part * 128, 128), 128)
                return tiles[slot - rank * n_dev, here, :].astype(jnp.float32)

            def add(p, values):
                slot = order[p]
                return tuple(value + read(slot, part) for part, value in enumerate(values))

            values = [front[part, rows(step), columns].astype(jnp.float32) for part in range(2)]
            for k in range(2):
                slot = order[first + k]
                here = jnp.full((128, 128), last - first, jnp.int32) > k
                values = [value + jnp.where(here, read(slot, part), 0.0) for part, value in enumerate(values)]
            for part, value in enumerate(values):
                near[part, rows(step), columns] = value.astype(jnp.bfloat16)

            @pl.when(last - first > 2)
            def _():
                more = lax.fori_loop(first + 2, last, add, tuple(values))
                for part, value in enumerate(more):
                    near[part, rows(step), columns] = value.astype(jnp.bfloat16)

        put(step).start()
        return carry

    def finish(step, carry):
        put(step).wait()
        return carry

    lax.fori_loop(0, rows_blocks, one, 0)
    lax.fori_loop(0, rows_blocks, finish, 0)


def body(front, child_tiles, tile_owner, tile_spot, tile_count, panel):
    n_row = lax.axis_size("row")
    n_dev = n_row * lax.axis_size("col")
    n_tiles = child_tiles.shape[0]
    tile = child_tiles.shape[2]
    height, width = front.shape[1:]
    rows_blocks, cols_blocks = height // tile, width // tile
    n_spots = rows_blocks * cols_blocks
    samples = panel.shape[2]
    f32, bf16, i32 = jnp.float32, jnp.bfloat16, jnp.int32
    smem = pl.BlockSpec(memory_space=pltpu.SMEM)
    vmem = pl.BlockSpec(memory_space=pltpu.VMEM)
    params = functools.partial(pltpu.CompilerParams, vmem_limit_bytes=VMEM_LIMIT)
    n_slots = 2 * n_dev
    message = 4 * tile + 8
    spot_range = pl.next_power_of_2(n_spots)

    packed = pl.pallas_call(
        functools.partial(pack, n_dev, spot_range),
        out_shape=jax.ShapeDtypeStruct((n_dev, message, tile), bf16),
        in_specs=[smem, smem, vmem],
        out_specs=vmem,
        scratch_shapes=[pltpu.SMEM((n_dev,), i32), pltpu.SMEM((n_slots,), i32)],
        compiler_params=params(),
        cost_estimate=pl.CostEstimate(flops=1 << 20, bytes_accessed=2 * n_dev * 65536, transcendentals=0),
        name="pack",
    )(tile_owner[:, 0] * spot_range + tile_spot, tile_count, child_tiles.reshape(n_tiles, 2 * tile, tile))
    got = lax.all_to_all(packed, BOTH, split_axis=0, concat_axis=0, tiled=True)

    spots = jnp.concatenate([got[:, 4 * tile, 0], got[:, 4 * tile, 1]]).astype(i32)
    slot = jnp.arange(n_slots, dtype=i32)
    spots = jnp.where(spots >= 0, spots, n_spots)
    key = spots * n_slots + slot
    place = jnp.sum((key[None, :] < key[:, None]).astype(i32), axis=1)
    order = jnp.sum(jnp.where(place[None, :] == jnp.arange(n_slots + 2)[:, None], slot[None, :], 0), axis=1)
    starts = jnp.sum((spots[None, :] < jnp.arange(n_spots + 1)[:, None]).astype(i32), axis=1)

    result = jax.ShapeDtypeStruct((2, height, width), bf16)
    assembled, near = pl.pallas_call(
        functools.partial(extend_add, n_dev, rows_blocks, cols_blocks),
        out_shape=(result, result),
        in_specs=[smem, smem, vmem, vmem],
        out_specs=(pl.BlockSpec(memory_space=pl.ANY), vmem),
        scratch_shapes=[pltpu.SemaphoreType.DMA((rows_blocks,))],
        compiler_params=params(),
        cost_estimate=pl.CostEstimate(flops=8 << 30, bytes_accessed=28 << 20, transcendentals=0),
        name="extend_add",
    )(order, starts, got, front)

    def product(p, a):
        return lax.dot_general(p, a, (((0,), (0,)), ((), ())), preferred_element_type=f32)

    real = product(panel[0], near[0]) + product(panel[1], near[1])
    imag = product(panel[0], near[1]) - product(panel[1], near[0])
    partial = jnp.stack([real.astype(bf16).reshape(n_row, -1, width), imag.astype(bf16).reshape(n_row, -1, width)], axis=1)
    arrived = lax.all_to_all(
        partial.reshape(n_row, 2 * samples // n_row, width), "row", split_axis=0, concat_axis=0, tiled=True
    )
    sample = arrived.astype(f32).sum(axis=0).reshape(2, samples // n_row, width)
    return assembled, sample


def solution(mesh):
    placed = (
        P(None, "row", "col"),
        P(BOTH, None, None, None),
        P(BOTH, None),
        P(BOTH),
        P(BOTH),
        P(None, "row", None),
    )
    return jax.shard_map(
        body,
        mesh=mesh,
        in_specs=placed,
        out_specs=(P(None, "row", "col"), P(None, "row", "col")),
        check_vma=False,
    )
```

```python
import functools

import jax
import jax.numpy as jnp
from jax import lax
from jax.experimental import pallas as pl
from jax.experimental.pallas import tpu as pltpu
from jax.sharding import PartitionSpec as P

BOTH = ("row", "col")
VMEM_LIMIT = 4 * 1024 * 1024


def pack(n_dev, n_spots, target, count, tiles, out, seen, spots):
    def clear(d, carry):
        seen[d] = 0
        for k in range(2):
            spots[d * 2 + k] = -1
        return carry

    lax.fori_loop(0, n_dev, clear, 0, unroll=8)

    def route(j, carry):
        to = target[j] // n_spots
        rank = seen[to]
        seen[to] = rank + 1
        spots[to * 2 + rank] = target[j] - to * n_spots
        out[to, pl.ds(pl.multiple_of(rank * 256, 256), 256), :] = tiles[j]
        return carry

    live = jnp.minimum(count[0], tiles.shape[0])
    lax.fori_loop(0, live // 4, lambda i, carry: functools.reduce(lambda c, u: route(i * 4 + u, c), range(4), carry), 0)
    lax.fori_loop(live // 4 * 4, live, route, 0)
    lane = lax.broadcasted_iota(jnp.int32, (8, 128), 1)

    def label(d, carry):
        row = jnp.where(lane == 0, spots[d * 2], jnp.where(lane == 1, spots[d * 2 + 1], 0))
        out[d, 512:520, :] = row.astype(jnp.float32).astype(jnp.bfloat16)
        return carry

    lax.fori_loop(0, n_dev, label, 0, unroll=4)


def extend_add(n_dev, rows_blocks, cols_blocks, order, starts, tiles, front, assembled, near, sem):
    def rows(step):
        return pl.ds(pl.multiple_of(step * 128, 128), 128)

    def put(step):
        return pltpu.make_async_copy(near.at[:, rows(step)], assembled.at[:, rows(step)], sem.at[step])

    def one(step, carry):
        for c in range(cols_blocks):
            first, last = starts[step * cols_blocks + c], starts[step * cols_blocks + c + 1]
            columns = slice(c * 128, (c + 1) * 128)

            def read(slot, part):
                rank = slot // n_dev
                here = pl.ds(pl.multiple_of(rank * 256 + part * 128, 128), 128)
                return tiles[slot - rank * n_dev, here, :].astype(jnp.float32)

            def add(p, values):
                slot = order[p]
                return tuple(value + read(slot, part) for part, value in enumerate(values))

            def add_two(i, values):
                p = first + i * 2
                slots = order[p], order[p + 1]
                return tuple(value + read(slots[0], part) + read(slots[1], part) for part, value in enumerate(values))

            values = tuple(front[part, rows(step), columns].astype(jnp.float32) for part in range(2))
            pairs = (last - first) // 2
            values = lax.fori_loop(0, pairs, add_two, values)
            values = lax.fori_loop(first + pairs * 2, last, add, values)
            for part, value in enumerate(values):
                near[part, rows(step), columns] = value.astype(jnp.bfloat16)

        put(step).start()
        return carry

    def finish(step, carry):
        put(step).wait()
        return carry

    lax.fori_loop(0, rows_blocks, one, 0)
    lax.fori_loop(0, rows_blocks, finish, 0)


def body(front, child_tiles, tile_owner, tile_spot, tile_count, panel):
    n_row = lax.axis_size("row")
    n_dev = n_row * lax.axis_size("col")
    n_tiles = child_tiles.shape[0]
    tile = child_tiles.shape[2]
    height, width = front.shape[1:]
    rows_blocks, cols_blocks = height // tile, width // tile
    n_spots = rows_blocks * cols_blocks
    samples = panel.shape[2]
    f32, bf16, i32 = jnp.float32, jnp.bfloat16, jnp.int32
    smem = pl.BlockSpec(memory_space=pltpu.SMEM)
    vmem = pl.BlockSpec(memory_space=pltpu.VMEM)
    params = functools.partial(pltpu.CompilerParams, vmem_limit_bytes=VMEM_LIMIT)
    n_slots = 2 * n_dev
    message = 4 * tile + 8
    spot_range = pl.next_power_of_2(n_spots)

    packed = pl.pallas_call(
        functools.partial(pack, n_dev, spot_range),
        out_shape=jax.ShapeDtypeStruct((n_dev, message, tile), bf16),
        in_specs=[smem, smem, vmem],
        out_specs=vmem,
        scratch_shapes=[pltpu.SMEM((n_dev,), i32), pltpu.SMEM((n_slots,), i32)],
        compiler_params=params(),
        cost_estimate=pl.CostEstimate(flops=1 << 20, bytes_accessed=2 * n_dev * 65536, transcendentals=0),
        name="pack",
    )(tile_owner[:, 0] * spot_range + tile_spot, tile_count, child_tiles.reshape(n_tiles, 2 * tile, tile))
    got = lax.all_to_all(packed, BOTH, split_axis=0, concat_axis=0, tiled=True)

    spots = jnp.concatenate([got[:, 4 * tile, 0], got[:, 4 * tile, 1]]).astype(i32)
    slot = jnp.arange(n_slots, dtype=i32)
    spots = jnp.where(spots >= 0, spots, n_spots)
    key = spots * n_slots + slot
    place = jnp.sum((key[None, :] < key[:, None]).astype(i32), axis=1)
    order = jnp.sum(jnp.where(place[None, :] == slot[:, None], slot[None, :], 0), axis=1)
    starts = jnp.sum((spots[None, :] < jnp.arange(n_spots + 1)[:, None]).astype(i32), axis=1)

    result = jax.ShapeDtypeStruct((2, height, width), bf16)
    assembled, near = pl.pallas_call(
        functools.partial(extend_add, n_dev, rows_blocks, cols_blocks),
        out_shape=(result, result),
        in_specs=[smem, smem, vmem, vmem],
        out_specs=(pl.BlockSpec(memory_space=pl.ANY), vmem),
        scratch_shapes=[pltpu.SemaphoreType.DMA((rows_blocks,))],
        compiler_params=params(),
        cost_estimate=pl.CostEstimate(flops=8 << 30, bytes_accessed=28 << 20, transcendentals=0),
        name="extend_add",
    )(order, starts, got, front)

    def product(p, a):
        return lax.dot_general(p, a, (((0,), (0,)), ((), ())), preferred_element_type=f32)

    real = product(panel[0], near[0]) + product(panel[1], near[1])
    imag = product(panel[0], near[1]) - product(panel[1], near[0])
    partial = jnp.stack([real.astype(bf16).reshape(n_row, -1, width), imag.astype(bf16).reshape(n_row, -1, width)], axis=1)
    arrived = lax.all_to_all(
        partial.reshape(n_row, 2 * samples // n_row, width), "row", split_axis=0, concat_axis=0, tiled=True
    )
    sample = arrived.astype(f32).sum(axis=0).reshape(2, samples // n_row, width)
    return assembled, sample


def solution(mesh):
    placed = (
        P(None, "row", "col"),
        P(BOTH, None, None, None),
        P(BOTH, None),
        P(BOTH),
        P(BOTH),
        P(None, "row", None),
    )
    return jax.shard_map(
        body,
        mesh=mesh,
        in_specs=placed,
        out_specs=(P(None, "row", "col"), P(None, "row", "col")),
        check_vma=False,
    )
```

```python
import functools

import jax
import jax.numpy as jnp
from jax import lax
from jax.experimental import pallas as pl
from jax.experimental.pallas import tpu as pltpu
from jax.sharding import PartitionSpec as P

BOTH = ("row", "col")
VMEM_LIMIT = 4 * 1024 * 1024


def pack(n_dev, n_spots, target, count, tiles, out, seen, spots):
    def clear(d, carry):
        seen[d] = 0
        for k in range(2):
            spots[d * 2 + k] = -1
        return carry

    lax.fori_loop(0, n_dev, clear, 0, unroll=8)

    def route(j, carry):
        to = target[j] // n_spots
        rank = seen[to]
        seen[to] = rank + 1
        spots[to * 2 + rank] = target[j] - to * n_spots
        out[to, pl.ds(pl.multiple_of(rank * 256, 256), 256), :] = tiles[j]
        return carry

    live = jnp.minimum(count[0], tiles.shape[0])
    lax.fori_loop(0, live // 4, lambda i, carry: functools.reduce(lambda c, u: route(i * 4 + u, c), range(4), carry), 0)
    lax.fori_loop(live // 4 * 4, live, route, 0)
    lane = lax.broadcasted_iota(jnp.int32, (8, 128), 1)

    def label(d, carry):
        row = jnp.where(lane == 0, spots[d * 2], jnp.where(lane == 1, spots[d * 2 + 1], 0))
        out[d, 512:520, :] = row.astype(jnp.float32).astype(jnp.bfloat16)
        return carry

    lax.fori_loop(0, n_dev, label, 0, unroll=4)


def extend_add(n_dev, rows_blocks, cols_blocks, order, starts, tiles, front, assembled, near, sem):
    def rows(step):
        return pl.ds(pl.multiple_of(step * 128, 128), 128)

    def put(step):
        return pltpu.make_async_copy(near.at[:, rows(step)], assembled.at[:, rows(step)], sem.at[step])

    def one(step, carry):
        for c in range(cols_blocks):
            first, last = starts[step * cols_blocks + c], starts[step * cols_blocks + c + 1]
            columns = slice(c * 128, (c + 1) * 128)

            def add(p, carry):
                slot, values = carry
                rank = slot // n_dev
                source = slot - rank * n_dev
                return order[p + 1], tuple(
                    value + tiles[source, pl.ds(pl.multiple_of(rank * 256 + part * 128, 128), 128), :].astype(jnp.float32)
                    for part, value in enumerate(values)
                )

            values = tuple(front[part, rows(step), columns].astype(jnp.float32) for part in range(2))
            for part, value in enumerate(lax.fori_loop(first, last, add, (order[first], values))[1]):
                near[part, rows(step), columns] = value.astype(jnp.bfloat16)
        put(step).start()
        return carry

    def finish(step, carry):
        put(step).wait()
        return carry

    lax.fori_loop(0, rows_blocks, one, 0)
    lax.fori_loop(0, rows_blocks, finish, 0)


def body(front, child_tiles, tile_owner, tile_spot, tile_count, panel):
    n_row = lax.axis_size("row")
    n_dev = n_row * lax.axis_size("col")
    n_tiles = child_tiles.shape[0]
    tile = child_tiles.shape[2]
    height, width = front.shape[1:]
    rows_blocks, cols_blocks = height // tile, width // tile
    n_spots = rows_blocks * cols_blocks
    samples = panel.shape[2]
    f32, bf16, i32 = jnp.float32, jnp.bfloat16, jnp.int32
    smem = pl.BlockSpec(memory_space=pltpu.SMEM)
    vmem = pl.BlockSpec(memory_space=pltpu.VMEM)
    params = functools.partial(pltpu.CompilerParams, vmem_limit_bytes=VMEM_LIMIT)
    n_slots = 2 * n_dev
    message = 4 * tile + 8
    spot_range = pl.next_power_of_2(n_spots)

    packed = pl.pallas_call(
        functools.partial(pack, n_dev, spot_range),
        out_shape=jax.ShapeDtypeStruct((n_dev, message, tile), bf16),
        in_specs=[smem, smem, vmem],
        out_specs=vmem,
        scratch_shapes=[pltpu.SMEM((n_dev,), i32), pltpu.SMEM((n_slots,), i32)],
        compiler_params=params(),
        cost_estimate=pl.CostEstimate(flops=1 << 20, bytes_accessed=2 * n_dev * 65536, transcendentals=0),
        name="pack",
    )(tile_owner[:, 0] * spot_range + tile_spot, tile_count, child_tiles.reshape(n_tiles, 2 * tile, tile))
    got = lax.all_to_all(packed, BOTH, split_axis=0, concat_axis=0, tiled=True)

    spots = jnp.concatenate([got[:, 4 * tile, 0], got[:, 4 * tile, 1]]).astype(i32)
    slot = jnp.arange(n_slots, dtype=i32)
    spots = jnp.where(spots >= 0, spots, n_spots)
    key = spots * n_slots + slot
    place = jnp.sum((key[None, :] < key[:, None]).astype(i32), axis=1)
    order = jnp.sum(jnp.where(place[None, :] == jnp.arange(n_slots + 1)[:, None], slot[None, :], 0), axis=1)
    starts = jnp.sum((spots[None, :] < jnp.arange(n_spots + 1)[:, None]).astype(i32), axis=1)

    result = jax.ShapeDtypeStruct((2, height, width), bf16)
    assembled, near = pl.pallas_call(
        functools.partial(extend_add, n_dev, rows_blocks, cols_blocks),
        out_shape=(result, result),
        in_specs=[smem, smem, vmem, vmem],
        out_specs=(pl.BlockSpec(memory_space=pl.ANY), vmem),
        scratch_shapes=[pltpu.SemaphoreType.DMA((rows_blocks,))],
        compiler_params=params(),
        cost_estimate=pl.CostEstimate(flops=8 << 30, bytes_accessed=28 << 20, transcendentals=0),
        name="extend_add",
    )(order, starts, got, front)

    def product(p, a):
        return lax.dot_general(p, a, (((0,), (0,)), ((), ())), preferred_element_type=f32)

    real = product(panel[0], near[0]) + product(panel[1], near[1])
    imag = product(panel[0], near[1]) - product(panel[1], near[0])
    partial = jnp.stack([real.astype(bf16).reshape(n_row, -1, width), imag.astype(bf16).reshape(n_row, -1, width)], axis=1)
    arrived = lax.all_to_all(
        partial.reshape(n_row, 2 * samples // n_row, width), "row", split_axis=0, concat_axis=0, tiled=True
    )
    sample = arrived.astype(f32).sum(axis=0).reshape(2, samples // n_row, width)
    return assembled, sample


def solution(mesh):
    placed = (
        P(None, "row", "col"),
        P(BOTH, None, None, None),
        P(BOTH, None),
        P(BOTH),
        P(BOTH),
        P(None, "row", None),
    )
    return jax.shard_map(
        body,
        mesh=mesh,
        in_specs=placed,
        out_specs=(P(None, "row", "col"), P(None, "row", "col")),
        check_vma=False,
    )
```
